32 devices in a mesh: dp: 8 (over z, x), fsdp: 4 (over y, core).
Axes of the slice: x: 2, y: 2, z: 4, core: 2. Of those that a mesh axis runs over, the one named last changes fastest.
Arguments:
- tokens: bfloat16 [16384, 640], P(('dp', 'fsdp')), may hold values from -6 to 6
- cotangent: bfloat16 [16384, 640], P(('dp', 'fsdp')), may hold values from -6 to 6
- segments: int32 [64, 256], P(('dp', 'fsdp')), may hold values from 0 to 7, never falling along the last dimension, each value on 1 to 128 neighbouring positions
- query_weight: float32 [1024, 640], P(('dp', 'fsdp')), may hold values from -0.25 to 0.25
- key_weight: float32 [640, 256], P(('dp', 'fsdp')), may hold values from -0.25 to 0.25
- value_weight: float32 [640, 256], P(('dp', 'fsdp')), may hold values from -0.25 to 0.25
- out_weight: float32 [1024, 640], P(('dp', 'fsdp')), may hold values from -0.1875 to 0.1875
- gate_weight: float32 [2048, 640], P(('dp', 'fsdp')), may hold values from -0.25 to 0.25
- up_weight: float32 [2048, 640], P(('dp', 'fsdp')), may hold values from -0.25 to 0.25
- down_weight: float32 [2048, 640], P(('dp', 'fsdp')), may hold values from -0.125 to 0.125
- norm_gains: float32 [3072], P(('dp', 'fsdp')), may hold values from 0.5 to 1.5
- query_state: float32 [1024, 640], P(('dp', 'fsdp')), may hold values from -224 to 224
- key_state: float32 [640, 256], P(('dp', 'fsdp')), may hold values from -224 to 224
- value_state: float32 [640, 256], P(('dp', 'fsdp')), may hold values from -224 to 224
- out_state: float32 [1024, 640], P(('dp', 'fsdp')), may hold values from -224 to 224
- gate_state: float32 [2048, 640], P(('dp', 'fsdp')), may hold values from -224 to 224
- up_state: float32 [2048, 640], P(('dp', 'fsdp')), may hold values from -224 to 224
- down_state: float32 [2048, 640], P(('dp', 'fsdp')), may hold values from -224 to 224
- gains_state: float32 [3072], P(('dp', 'fsdp')), may hold values from -224 to 224
Outputs:
- block_out: bfloat16 [16384, 640], P(('dp', 'fsdp'))
- tokens_grad: bfloat16 [16384, 640], P(('dp', 'fsdp'))
- query_grad: float32 [1024, 640], P(('dp', 'fsdp'))
- key_grad: float32 [640, 256], P(('dp', 'fsdp'))
- value_grad: float32 [640, 256], P(('dp', 'fsdp'))
- out_grad: float32 [1024, 640], P(('dp', 'fsdp'))
- gate_grad: float32 [2048, 640], P(('dp', 'fsdp'))
- up_grad: float32 [2048, 640], P(('dp', 'fsdp'))
- down_grad: float32 [2048, 640], P(('dp', 'fsdp'))
- gains_grad: float32 [3072], P(('dp', 'fsdp'))
- query_new: float32 [1024, 640], P(('dp', 'fsdp'))
- key_new: float32 [640, 256], P(('dp', 'fsdp'))
- value_new: float32 [640, 256], P(('dp', 'fsdp'))
- out_new: float32 [1024, 640], P(('dp', 'fsdp'))
- gate_new: float32 [2048, 640], P(('dp', 'fsdp'))
- up_new: float32 [2048, 640], P(('dp', 'fsdp'))
- down_new: float32 [2048, 640], P(('dp', 'fsdp'))
- gains_new: float32 [3072], P(('dp', 'fsdp'))
- query_moment: float32 [1024, 640], P(('dp', 'fsdp'))
- key_moment: float32 [640, 256], P(('dp', 'fsdp'))
- value_moment: float32 [640, 256], P(('dp', 'fsdp'))
- out_moment: float32 [1024, 640], P(('dp', 'fsdp'))
- gate_moment: float32 [2048, 640], P(('dp', 'fsdp'))
- up_moment: float32 [2048, 640], P(('dp', 'fsdp'))
- down_moment: float32 [2048, 640], P(('dp', 'fsdp'))
- gains_moment: float32 [3072], P(('dp', 'fsdp'))
The draws below stay inside these ranges and needn't reach their ends.
Inputs may be any that keep to these rules, and one draw needn't show every extreme that they name: `segments`: segment numbers never fall along a row; the tokens of one number form one sequence.
All inputs are finite; a program needn't handle non-finite values.
Results may differ from the reference program's by a relative error of at most 0.015.
The reference program's roundings to bfloat16 on the way count: a program that leaves them out, or rounds other values in their place, can miss the bound.
Values may be sent and summed in bfloat16 or wider, within the bound.
A program may use at most 320 MiB of HBM per device.

```python
import math
import jax
import jax.numpy as jnp
import numpy as np
from jax import lax

D = 640
HEADS = 4
HD = 256
FF = 2048
CAP = 256
SEQS = 8
NS_ITERS = 5
HQ = 1024
GN = 3072
TOKENS = 16384
BLOCKS = 64


def level_of(own_key, shape, cuts, low, largest):
    loudness, own = 1.0, jax.random.fold_in(own_key, 6)
    for dim, shards_of in cuts:
        steps = jnp.exp(jax.random.uniform(jax.random.fold_in(own, dim), (shards_of,), jnp.float32, low / len(cuts), largest / len(cuts)))
        loudness = loudness * jnp.repeat(steps, shape[dim] // shards_of).reshape([-1 if axis == dim else 1 for axis in range(len(shape))])
    return loudness


def length_profile(number_of, total, bound, slope):
    portions = [(1 << 20) // math.isqrt(grade ** slope) + 1 for grade in range(2, number_of + 1)]
    surplus, given = total - bound - (number_of - 1), [1] * (number_of - 1)
    while surplus > 0:
        free = [i for i in range(number_of - 1) if given[i] < bound]
        mass, left = sum([portions[i] for i in free]), surplus
        for i in free:
            more = min(bound - given[i], max(1, left * portions[i] // mass), surplus)
            given[i] = given[i] + more
            surplus = surplus - more
    return np.array([bound] + given)


def ragged(rng, count, total, bound, slope):
    if count == 2:
        one = jax.random.randint(rng, (), max(1, total - bound), min(bound, total - 1) + 1)
        return jnp.stack([one, total - one])
    sizes = jnp.asarray(length_profile(count, total, bound, slope), jnp.int32)
    twos = (count - 1) // 2
    giver, taker = sizes[1:1 + 2 * twos:2], sizes[2:2 + 2 * twos:2]
    room = jnp.minimum(giver - 1, bound - taker)
    passed = jax.random.randint(jax.random.fold_in(rng, 1), (twos,), 0, 1 << 20) % (room + 1)
    sizes = sizes.at[1:1 + 2 * twos:2].set(giver - passed).at[2:2 + 2 * twos:2].set(taker + passed)
    return sizes[jax.random.permutation(jax.random.fold_in(rng, 2), count)]


def noise(own_key, dims, scale, limit, cuts=(), kind=jnp.bfloat16):
    entries = scale * jax.random.normal(own_key, dims, jnp.float32)
    if cuts:
        entries = entries * level_of(own_key, dims, cuts, -0.22, 0.18)
    return jnp.clip(entries, -limit, limit).astype(kind)


def setup_inputs(seed: int = 0) -> dict:
    seeds = jax.random.split(jax.random.key(seed), 20)
    return {
        "tokens": noise(seeds[0], (TOKENS, D), 1.0, 6.0, ((0, 32),)),
        "cotangent": noise(seeds[1], (TOKENS, D), 1.0, 6.0, ((0, 32),)),
        "segments": jax.vmap(lambda own: jnp.searchsorted(jnp.cumsum(ragged(own, SEQS, CAP, CAP // 2, 2)), jnp.arange(CAP), side="right"))(jax.random.split(seeds[2], BLOCKS)).reshape((BLOCKS, CAP)).astype(jnp.int32),
        "query_weight": noise(seeds[3], (HQ, D), D ** -0.5, 0.25, ((0, 32),), jnp.float32),
        "key_weight": noise(seeds[4], (D, HD), D ** -0.5, 0.25, ((0, 32),), jnp.float32),
        "value_weight": noise(seeds[5], (D, HD), D ** -0.5, 0.25, ((0, 32),), jnp.float32),
        "out_weight": noise(seeds[6], (HQ, D), HQ ** -0.5, 0.1875, ((0, 32),), jnp.float32),
        "gate_weight": noise(seeds[7], (FF, D), D ** -0.5, 0.25, ((0, 32),), jnp.float32),
        "up_weight": noise(seeds[8], (FF, D), D ** -0.5, 0.25, ((0, 32),), jnp.float32),
        "down_weight": noise(seeds[9], (FF, D), FF ** -0.5, 0.125, ((0, 32),), jnp.float32),
        "norm_gains": jnp.clip(1.0 + 0.1 * jax.random.normal(seeds[10], (GN,), jnp.float32), 0.5, 1.5),
        "query_state": noise(seeds[11], (HQ, D), (0.3 * TOKENS ** 0.5), 224.0, ((0, 32),), jnp.float32),
        "key_state": noise(seeds[12], (D, HD), (0.3 * TOKENS ** 0.5), 224.0, ((0, 32),), jnp.float32),
        "value_state": noise(seeds[13], (D, HD), (0.3 * TOKENS ** 0.5), 224.0, ((0, 32),), jnp.float32),
        "out_state": noise(seeds[14], (HQ, D), (0.3 * TOKENS ** 0.5), 224.0, ((0, 32),), jnp.float32),
        "gate_state": noise(seeds[15], (FF, D), (0.3 * TOKENS ** 0.5), 224.0, ((0, 32),), jnp.float32),
        "up_state": noise(seeds[16], (FF, D), (0.3 * TOKENS ** 0.5), 224.0, ((0, 32),), jnp.float32),
        "down_state": noise(seeds[17], (FF, D), (0.3 * TOKENS ** 0.5), 224.0, ((0, 32),), jnp.float32),
        "gains_state": noise(seeds[18], (GN,), (0.3 * TOKENS ** 0.5), 224.0, ((0, 32),), jnp.float32),
    }


EPSILON = 1e-06
THETA = 1000000.0
MOMENTUM = 0.95
LEARN_RATE = 0.05
NS_FIRST = 3.4445
NS_SECOND = -4.775
NS_THIRD = 2.0315
HIGHEST = lax.Precision.HIGHEST
MASKED = -1e+30

def dot_plain(left, right):
    return jnp.dot(left, right, preferred_element_type=jnp.float32)

def dot_right_t(left, right):
    return lax.dot_general(left, right, (((1,), (1,)), ((), ())), preferred_element_type=jnp.float32)

def dot_left_t(left, right):
    return lax.dot_general(left, right, (((0,), (0,)), ((), ())), preferred_element_type=jnp.float32)

def norm_rows(values, gain):
    return values * lax.rsqrt(lax.optimization_barrier(jnp.mean(values * values, axis=-1, keepdims=True)) + EPSILON) * gain

def rotary(values, cosine, sine):
    middle = values.shape[-1] // 2
    first_half = values[..., :middle]
    second_half = values[..., middle:]
    return jnp.concatenate([first_half * cosine - second_half * sine, second_half * cosine + first_half * sine], axis=-1)

def rotary_tables(segment, head_size):
    length = segment.shape[0]
    starts = lax.optimization_barrier(jnp.sum((segment[None, :] < segment[:, None]).astype(jnp.int32), axis=1))
    places = (jnp.arange(length, dtype=jnp.int32) - starts).astype(jnp.float32)
    frequency = jnp.exp(-math.log(THETA) * 2.0 * jnp.arange(head_size // 2, dtype=jnp.float32) / head_size)
    angles = places[:, None] * frequency[None, :]
    return (jnp.cos(angles), jnp.sin(angles))

def allowed_pairs(segment):
    length = segment.shape[0]
    positions = jnp.arange(length, dtype=jnp.int32)
    same_doc = segment[:, None] == segment[None, :]
    return jnp.logical_and(same_doc, positions[None, :] <= positions[:, None])

def split_gains(gain_vec, width, head_size):
    return (gain_vec[:width], gain_vec[width:2 * width], gain_vec[2 * width:3 * width], gain_vec[3 * width:4 * width], gain_vec[4 * width:4 * width + head_size], gain_vec[4 * width + head_size:])

def query_rotated(query, gain, cosine, sine):
    length = query.shape[0]
    shaped = query.reshape(length, HEADS, query.shape[1] // HEADS)
    return rotary(norm_rows(shaped, gain), cosine[:, None, :], sine[:, None, :])

def key_rotated(key_rows, gain, cosine, sine):
    return rotary(norm_rows(key_rows, gain), cosine, sine)

def attention_scores(query_bf, key_bf, allowed):
    scale = query_bf.shape[-1] ** (-0.5)
    products = jnp.einsum('thd,sd->hts', query_bf.astype(jnp.float32), key_bf.astype(jnp.float32)) * scale
    return jnp.where(allowed[None], products, MASKED)

def gelu_product(gate, upward):
    return jax.nn.gelu(gate, approximate=True) * upward

def forward(rows_in, segment, weights, gain_vec):
    query_w, key_w, value_w, out_w, gate_w, up_w, down_w = weights
    width = rows_in.shape[1]
    head_size = key_w.shape[1]
    gain_in, gain_attn, gain_ff, gain_post, gain_query, gain_key = split_gains(gain_vec, width, head_size)
    x_rows = rows_in.astype(jnp.float32)
    normed = norm_rows(x_rows, gain_in).astype(jnp.bfloat16)
    query = dot_right_t(normed, query_w)
    key_rows = dot_plain(normed, key_w)
    value = dot_plain(normed, value_w).astype(jnp.bfloat16)
    cosine, sine = rotary_tables(segment, head_size)
    query_bf = query_rotated(query, gain_query, cosine, sine).astype(jnp.bfloat16)
    key_bf = key_rotated(key_rows, gain_key, cosine, sine).astype(jnp.bfloat16)
    allowed = allowed_pairs(segment)
    scores = attention_scores(query_bf, key_bf, allowed)
    peak = lax.optimization_barrier(jnp.max(scores, axis=-1, keepdims=True))
    log_total = peak + jnp.log(lax.optimization_barrier(jnp.sum(jnp.exp(scores - peak), axis=-1, keepdims=True)))
    probs = jnp.exp(scores - log_total).astype(jnp.bfloat16)
    mixed = jnp.einsum('hts,sd->thd', probs.astype(jnp.float32), value.astype(jnp.float32))
    mixed = mixed.astype(jnp.bfloat16).reshape(rows_in.shape[0], -1)
    attn = dot_plain(mixed, out_w)
    hidden = x_rows + norm_rows(attn, gain_attn)
    ff_in = norm_rows(hidden, gain_ff).astype(jnp.bfloat16)
    gate = dot_right_t(ff_in, gate_w)
    upward = dot_right_t(ff_in, up_w)
    act = gelu_product(gate, upward).astype(jnp.bfloat16)
    ff_out = dot_plain(act, down_w)
    result = (hidden + norm_rows(ff_out, gain_post)).astype(jnp.bfloat16)
    saved = (x_rows, normed, query, key_rows, value, query_bf, key_bf, allowed, cosine, sine, log_total, mixed, attn, hidden, ff_in, gate, upward, act, ff_out)
    return (result, saved)

def backward(saved, cot_rows, weights, gain_vec):
    x_rows, normed, query, key_rows, value, query_bf, key_bf, allowed, cosine, sine, log_total, mixed, attn, hidden, ff_in, gate, upward, act, ff_out = saved
    query_w, key_w, value_w, out_w, gate_w, up_w, down_w = weights
    width = x_rows.shape[1]
    head_size = key_w.shape[1]
    gain_in, gain_attn, gain_ff, gain_post, gain_query, gain_key = split_gains(gain_vec, width, head_size)
    d_output = cot_rows.astype(jnp.float32)
    unused, pullback = jax.vjp(norm_rows, ff_out, gain_post)
    d_ffout, dg_post = pullback(d_output)
    d_ffout = d_ffout.astype(jnp.bfloat16)
    down_grad = dot_left_t(act, d_ffout)
    d_act = dot_right_t(d_ffout, down_w)
    unused, pullback = jax.vjp(gelu_product, gate, upward)
    d_gate, d_upward = pullback(d_act)
    d_gate = d_gate.astype(jnp.bfloat16)
    d_upward = d_upward.astype(jnp.bfloat16)
    gate_grad = dot_left_t(d_gate, ff_in)
    up_grad = dot_left_t(d_upward, ff_in)
    d_ffin = dot_plain(d_gate, gate_w) + dot_plain(d_upward, up_w)
    unused, pullback = jax.vjp(norm_rows, hidden, gain_ff)
    d_inner, dg_ff = pullback(d_ffin)
    d_hidden = d_output + d_inner
    unused, pullback = jax.vjp(norm_rows, attn, gain_attn)
    d_attn, dg_attn = pullback(d_hidden)
    d_attn = d_attn.astype(jnp.bfloat16)
    out_grad = dot_left_t(mixed, d_attn)
    d_mixed = dot_right_t(d_attn, out_w).astype(jnp.bfloat16).reshape(x_rows.shape[0], HEADS, head_size)
    scores = attention_scores(query_bf, key_bf, allowed)
    probs_full = jnp.exp(scores - log_total)
    probs = probs_full.astype(jnp.bfloat16)
    d_value = jnp.einsum('hts,thd->sd', probs.astype(jnp.float32), d_mixed.astype(jnp.float32)).astype(jnp.bfloat16)
    d_probs = jnp.einsum('thd,sd->hts', d_mixed.astype(jnp.float32), value.astype(jnp.float32))
    row_dot = lax.optimization_barrier(jnp.sum(probs_full * d_probs, axis=-1, keepdims=True))
    d_scores = (probs_full * (d_probs - row_dot) * head_size ** (-0.5)).astype(jnp.bfloat16)
    d_qrot = jnp.einsum('hts,sd->thd', d_scores.astype(jnp.float32), key_bf.astype(jnp.float32))
    d_krot = jnp.einsum('hts,thd->sd', d_scores.astype(jnp.float32), query_bf.astype(jnp.float32))
    unused, pullback = jax.vjp(lambda values, gain: query_rotated(values, gain, cosine, sine), query, gain_query)
    d_query, dg_query = pullback(d_qrot)
    unused, pullback = jax.vjp(lambda values, gain: key_rotated(values, gain, cosine, sine), key_rows, gain_key)
    d_key, dg_key = pullback(d_krot)
    d_query = d_query.astype(jnp.bfloat16)
    d_key = d_key.astype(jnp.bfloat16)
    query_grad = dot_left_t(d_query, normed)
    key_grad = dot_left_t(normed, d_key)
    value_grad = dot_left_t(normed, d_value)
    d_normed = dot_plain(d_query, query_w) + dot_right_t(d_key, key_w) + dot_right_t(d_value, value_w)
    unused, pullback = jax.vjp(norm_rows, x_rows, gain_in)
    d_inputs, dg_in = pullback(d_normed)
    grad_rows = (d_hidden + d_inputs).astype(jnp.bfloat16)
    gain_grad = jnp.concatenate([dg_in, dg_attn, dg_ff, dg_post, dg_query, dg_key])
    grads = (query_grad, key_grad, value_grad, out_grad, gate_grad, up_grad, down_grad)
    return (grad_rows, grads, gain_grad)

def orthogonalize(matrix):
    iterate = matrix / (jnp.sqrt(jnp.sum(matrix * matrix)) + 1e-07)
    for iteration in range(NS_ITERS):
        gram_matrix = jnp.dot(iterate.T, iterate, precision=HIGHEST, preferred_element_type=jnp.float32)
        polynomial = NS_SECOND * gram_matrix + NS_THIRD * jnp.dot(gram_matrix, gram_matrix, precision=HIGHEST, preferred_element_type=jnp.float32)
        iterate = NS_FIRST * iterate + jnp.dot(iterate, polynomial, precision=HIGHEST, preferred_element_type=jnp.float32)
    return iterate

def reference(tokens, cotangent, segments, query_weight, key_weight, value_weight, out_weight, gate_weight, up_weight, down_weight, norm_gains, query_state, key_state, value_state, out_state, gate_state, up_state, down_state, gains_state):
    masters = (query_weight, key_weight, value_weight, out_weight, gate_weight, up_weight, down_weight)
    states = (query_state, key_state, value_state, out_state, gate_state, up_state, down_state)
    weights = tuple((matrix.astype(jnp.bfloat16) for matrix in masters))
    gain_vec = lax.optimization_barrier(norm_gains.astype(jnp.bfloat16)).astype(jnp.float32)
    token_blocks = tokens.reshape(BLOCKS, CAP, D)
    cot_blocks = cotangent.reshape(BLOCKS, CAP, D)

    def per_block(carry, inputs):
        rows_in, cot_rows, segment = inputs
        result, saved = forward(rows_in, segment, weights, gain_vec)
        grad_rows, grads, gain_grad = backward(saved, cot_rows, weights, gain_vec)
        summed = tuple((total + extra for total, extra in zip(carry[0], grads)))
        return ((summed, carry[1] + gain_grad), (result, grad_rows))
    starting = (tuple((jnp.zeros(matrix.shape, jnp.float32) for matrix in masters)), jnp.zeros(norm_gains.shape, jnp.float32))
    (grad_list, gains_grad), (results, grad_rows) = lax.scan(per_block, starting, (token_blocks, cot_blocks, segments))
    block_out = results.reshape(TOKENS, D)
    tokens_grad = grad_rows.reshape(TOKENS, D)
    updated = []
    moments = []
    for number in range(7):
        moment = MOMENTUM * states[number] + grad_list[number]
        orthogonal = orthogonalize(moment)
        rows_all, cols_all = moment.shape
        factor = LEARN_RATE * 0.2 * math.sqrt(max(rows_all, cols_all))
        updated.append(masters[number] - factor * orthogonal)
        moments.append(moment)
    gains_moment = MOMENTUM * gains_state + gains_grad
    gains_new = norm_gains - 0.1 / math.sqrt(TOKENS) * gains_moment
    return (block_out, tokens_grad, grad_list[0], grad_list[1], grad_list[2], grad_list[3], grad_list[4], grad_list[5], grad_list[6], gains_grad, updated[0], updated[1], updated[2], updated[3], updated[4], updated[5], updated[6], gains_new, moments[0], moments[1], moments[2], moments[3], moments[4], moments[5], moments[6], gains_moment)
```

```python
import math

import jax
import jax.numpy as jnp
from jax import lax
from jax.sharding import PartitionSpec as P

D = 640
HEADS = 4
HD = 256
FF = 2048
NS_ITERS = 5


EPSILON = 1e-06
THETA = 1000000.0
MOMENTUM = 0.95
LEARN_RATE = 0.05
NS_FIRST = 3.4445
NS_SECOND = -4.775
NS_THIRD = 2.0315
HIGHEST = lax.Precision.HIGHEST
MASKED = -1e30


def dot_plain(left, right):
    return jnp.dot(left, right, preferred_element_type=jnp.float32)


def dot_right_t(left, right):
    return lax.dot_general(
        left, right, (((1,), (1,)), ((), ())), preferred_element_type=jnp.float32
    )


def dot_left_t(left, right):
    return lax.dot_general(
        left, right, (((0,), (0,)), ((), ())), preferred_element_type=jnp.float32
    )


def norm_rows(values, gain):
    return values * lax.rsqrt(jnp.mean(values * values, axis=-1, keepdims=True) + EPSILON) * gain


def rotary(values, cosine, sine):
    middle = values.shape[-1] // 2
    first_half = values[..., :middle]
    second_half = values[..., middle:]
    return jnp.concatenate(
        [first_half * cosine - second_half * sine, second_half * cosine + first_half * sine],
        axis=-1,
    )


def rotary_tables(segment, head_size):
    length = segment.shape[1]
    starts = jnp.sum((segment[:, None, :] < segment[:, :, None]).astype(jnp.int32), axis=2)
    places = (jnp.arange(length, dtype=jnp.int32)[None] - starts).astype(jnp.float32)
    frequency = jnp.exp(
        -math.log(THETA) * 2.0 * jnp.arange(head_size // 2, dtype=jnp.float32) / head_size
    )
    angles = places.reshape(-1)[:, None] * frequency[None, :]
    return (jnp.cos(angles), jnp.sin(angles))


def allowed_pairs(segment):
    length = segment.shape[1]
    positions = jnp.arange(length, dtype=jnp.int32)
    same_doc = segment[:, :, None] == segment[:, None, :]
    return jnp.logical_and(same_doc, (positions[None, :] <= positions[:, None])[None])


def split_gains(gain_vec, width, head_size):
    return (
        gain_vec[:width],
        gain_vec[width : 2 * width],
        gain_vec[2 * width : 3 * width],
        gain_vec[3 * width : 4 * width],
        gain_vec[4 * width : 4 * width + head_size],
        gain_vec[4 * width + head_size :],
    )


def query_rotated(query, gain, cosine, sine):
    length = query.shape[0]
    shaped = query.reshape(length, HEADS, query.shape[1] // HEADS)
    return rotary(norm_rows(shaped, gain), cosine[:, None, :], sine[:, None, :])


def key_rotated(key_rows, gain, cosine, sine):
    return rotary(norm_rows(key_rows, gain), cosine, sine)


def attention_scores(query_bf, key_bf, allowed):
    scale = query_bf.shape[-1] ** (-0.5)
    products = (
        jnp.einsum("bthd,bsd->bhts", query_bf, key_bf, preferred_element_type=jnp.float32) * scale
    )
    return jnp.where(allowed[:, None], products, MASKED)


def gelu_product(gate, upward):
    return jax.nn.gelu(gate, approximate=True) * upward


def block_step(rows_in, cot_rows, segment, weights, gain_vec):
    query_w, key_w, value_w, out_w, gate_w, up_w, down_w = weights
    batches, length = segment.shape
    total, width = rows_in.shape
    head_size = key_w.shape[1]
    gain_in, gain_attn, gain_ff, gain_post, gain_query, gain_key = split_gains(
        gain_vec, width, head_size
    )
    x_rows = rows_in.astype(jnp.float32)
    normed = norm_rows(x_rows, gain_in).astype(jnp.bfloat16)
    query = dot_right_t(normed, query_w)
    key_rows = dot_plain(normed, key_w)
    value = dot_plain(normed, value_w).astype(jnp.bfloat16)
    cosine, sine = rotary_tables(segment, head_size)
    query_bf = query_rotated(query, gain_query, cosine, sine).astype(jnp.bfloat16)
    query_bf = query_bf.reshape(batches, length, HEADS, head_size)
    key_bf = key_rotated(key_rows, gain_key, cosine, sine).astype(jnp.bfloat16)
    key_bf = key_bf.reshape(batches, length, head_size)
    value_b = value.reshape(batches, length, head_size)
    allowed = allowed_pairs(segment)
    scores = attention_scores(query_bf, key_bf, allowed)
    peak = jnp.max(scores, axis=-1, keepdims=True)
    log_total = peak + jnp.log(jnp.sum(jnp.exp(scores - peak), axis=-1, keepdims=True))
    probs_full = jnp.exp(scores - log_total)
    probs = probs_full.astype(jnp.bfloat16)
    mixed = jnp.einsum("bhts,bsd->bthd", probs, value_b, preferred_element_type=jnp.float32)
    mixed = mixed.astype(jnp.bfloat16).reshape(total, -1)
    attn = dot_plain(mixed, out_w)
    hidden = x_rows + norm_rows(attn, gain_attn)
    ff_in = norm_rows(hidden, gain_ff).astype(jnp.bfloat16)
    gate = dot_right_t(ff_in, gate_w)
    upward = dot_right_t(ff_in, up_w)
    act = gelu_product(gate, upward).astype(jnp.bfloat16)
    ff_out = dot_plain(act, down_w)
    result = (hidden + norm_rows(ff_out, gain_post)).astype(jnp.bfloat16)

    d_output = cot_rows.astype(jnp.float32)
    unused, pullback = jax.vjp(norm_rows, ff_out, gain_post)
    d_ffout, dg_post = pullback(d_output)
    d_ffout = d_ffout.astype(jnp.bfloat16)
    down_grad = dot_left_t(act, d_ffout)
    d_act = dot_right_t(d_ffout, down_w)
    unused, pullback = jax.vjp(gelu_product, gate, upward)
    d_gate, d_upward = pullback(d_act)
    d_gate = d_gate.astype(jnp.bfloat16)
    d_upward = d_upward.astype(jnp.bfloat16)
    gate_grad = dot_left_t(d_gate, ff_in)
    up_grad = dot_left_t(d_upward, ff_in)
    d_ffin = dot_plain(d_gate, gate_w) + dot_plain(d_upward, up_w)
    unused, pullback = jax.vjp(norm_rows, hidden, gain_ff)
    d_inner, dg_ff = pullback(d_ffin)
    d_hidden = d_output + d_inner
    unused, pullback = jax.vjp(norm_rows, attn, gain_attn)
    d_attn, dg_attn = pullback(d_hidden)
    d_attn = d_attn.astype(jnp.bfloat16)
    out_grad = dot_left_t(mixed, d_attn)
    d_mixed = dot_right_t(d_attn, out_w).astype(jnp.bfloat16)
    d_mixed = d_mixed.reshape(batches, length, HEADS, head_size)
    d_value = jnp.einsum(
        "bhts,bthd->bsd", probs, d_mixed, preferred_element_type=jnp.float32
    ).astype(jnp.bfloat16)
    d_probs = jnp.einsum("bthd,bsd->bhts", d_mixed, value_b, preferred_element_type=jnp.float32)
    row_dot = jnp.sum(probs_full * d_probs, axis=-1, keepdims=True)
    d_scores = (probs_full * (d_probs - row_dot) * head_size ** (-0.5)).astype(jnp.bfloat16)
    d_qrot = jnp.einsum("bhts,bsd->bthd", d_scores, key_bf, preferred_element_type=jnp.float32)
    d_krot = jnp.einsum("bhts,bthd->bsd", d_scores, query_bf, preferred_element_type=jnp.float32)
    d_qrot = d_qrot.reshape(total, HEADS, head_size)
    d_krot = d_krot.reshape(total, head_size)
    d_value = d_value.reshape(total, head_size)
    unused, pullback = jax.vjp(
        lambda values, gain: query_rotated(values, gain, cosine, sine), query, gain_query
    )
    d_query, dg_query = pullback(d_qrot)
    unused, pullback = jax.vjp(
        lambda values, gain: key_rotated(values, gain, cosine, sine), key_rows, gain_key
    )
    d_key, dg_key = pullback(d_krot)
    d_query = d_query.astype(jnp.bfloat16)
    d_key = d_key.astype(jnp.bfloat16)
    query_grad = dot_left_t(d_query, normed)
    key_grad = dot_left_t(normed, d_key)
    value_grad = dot_left_t(normed, d_value)
    d_normed = (
        dot_plain(d_query, query_w) + dot_right_t(d_key, key_w) + dot_right_t(d_value, value_w)
    )
    unused, pullback = jax.vjp(norm_rows, x_rows, gain_in)
    d_inputs, dg_in = pullback(d_normed)
    grad_rows = (d_hidden + d_inputs).astype(jnp.bfloat16)
    gain_grad = jnp.concatenate([dg_in, dg_attn, dg_ff, dg_post, dg_query, dg_key])
    grads = (query_grad, key_grad, value_grad, out_grad, gate_grad, up_grad, down_grad)
    return (result, grad_rows, grads, gain_grad)


def dot_fine(left, right):
    return jnp.dot(
        left, right, precision=lax.Precision.HIGH, preferred_element_type=jnp.float32
    )


def polar_factor(rows_all):
    gram = dot_left_t(rows_all, rows_all)
    size = gram.shape[0]
    eye = jnp.arange(size)[:, None] == jnp.arange(size)[None, :]
    inverse = 1.0 / (jnp.sqrt(jnp.sum(jnp.where(eye, gram, 0.0))) + 1e-07)
    gram = gram * (inverse * inverse)
    product = None
    for iteration in range(NS_ITERS):
        square = dot_fine(gram, gram)
        poly = NS_SECOND * gram + NS_THIRD * square + jnp.where(eye, NS_FIRST, 0.0)
        product = poly if product is None else dot_fine(product, poly)
        if iteration + 1 < NS_ITERS:
            cubic = NS_FIRST * gram + NS_SECOND * square + NS_THIRD * dot_fine(gram, square)
            gram = dot_fine(cubic, poly)
    return product * inverse


def as_rows(shard, width):
    return shard.reshape(-1, width)


def pad_to(piece, rows, cols):
    return jnp.pad(piece, ((0, rows - piece.shape[0]), (0, cols - piece.shape[1])))


def shards(
    tokens,
    cotangent,
    segments,
    query_weight,
    key_weight,
    value_weight,
    out_weight,
    gate_weight,
    up_weight,
    down_weight,
    norm_gains,
    query_state,
    key_state,
    value_state,
    out_state,
    gate_state,
    up_state,
    down_state,
    gains_state,
):
    axes = ("dp", "fsdp")
    groups = lax.axis_size("dp")
    devices_all = lax.axis_size("fsdp") * groups
    width = tokens.shape[1]
    masters = (
        query_weight,
        key_weight,
        value_weight,
        out_weight,
        gate_weight,
        up_weight,
        down_weight,
    )
    states = (query_state, key_state, value_state, out_state, gate_state, up_state, down_state)
    sizes = [matrix.size // width for matrix in masters]
    starts = [sum(sizes[:number]) for number in range(8)]
    gain_rows = norm_gains.shape[0]
    padded_rows = -(-(starts[7] + 1) // 16) * 16

    def pack(pieces, gains, lead):
        filler = jnp.zeros(lead + ((padded_rows - starts[7]) * width - gain_rows,), jnp.bfloat16)
        last = jnp.concatenate([gains, filler], axis=-1)
        last = last.reshape(lead + (padded_rows - starts[7], width))
        return jnp.concatenate(list(pieces) + [last], axis=len(lead))

    packed = pack(
        [as_rows(matrix.astype(jnp.bfloat16), width) for matrix in masters],
        norm_gains.astype(jnp.bfloat16),
        (),
    )
    gathered = lax.all_gather(packed, axes, axis=0, tiled=False)
    weights = tuple(
        gathered[:, starts[number] : starts[number + 1]].reshape(-1, masters[number].shape[1])
        for number in range(7)
    )
    gain_vec = gathered[:, starts[7], :gain_rows].reshape(-1).astype(jnp.float32)
    block_out, tokens_grad, grads, gain_grad = block_step(
        tokens, cotangent, segments, weights, gain_vec
    )
    sends = pack(
        [grad.astype(jnp.bfloat16).reshape(devices_all, -1, width) for grad in grads],
        gain_grad.astype(jnp.bfloat16).reshape(devices_all, gain_rows),
        (devices_all,),
    )
    summed = lax.psum_scatter(
        sends.reshape(devices_all * padded_rows, width), axes, scatter_dimension=0, tiled=True
    )
    grad_list = [
        summed[starts[number] : starts[number + 1]]
        .reshape(masters[number].shape)
        .astype(jnp.float32)
        for number in range(7)
    ]
    gains_grad = summed[starts[7], :gain_rows].astype(jnp.float32)
    moments = [MOMENTUM * state + grad for state, grad in zip(states, grad_list)]
    gains_moment = MOMENTUM * gains_state + gains_grad

    slots = -(-7 // groups)
    tile = max(matrix.shape[0] for matrix in masters)
    blank = jnp.zeros((tile, width), jnp.bfloat16)
    chunks = [pad_to(moment.astype(jnp.bfloat16), tile, width) for moment in moments]
    chunks = chunks + [blank] * (groups * slots - 7)
    outgoing = jnp.stack(chunks, axis=0)
    mine = lax.all_to_all(outgoing, "dp", split_axis=0, concat_axis=0, tiled=True)
    mine = mine.reshape(groups, slots, tile, width).swapaxes(0, 1).reshape(slots, -1, width)
    whole = lax.all_gather(mine, "fsdp", axis=1, tiled=True)
    ortho = []
    for place in range(slots):
        factor = polar_factor(whole[place]).astype(jnp.bfloat16)
        ortho.append(dot_plain(mine[place], factor).astype(jnp.bfloat16))
    ortho = jnp.stack(ortho, axis=0).reshape(slots, groups, tile, width).swapaxes(0, 1)
    back = lax.all_to_all(
        ortho.reshape(groups * slots, tile, width), "dp", split_axis=0, concat_axis=0, tiled=True
    )
    updated = []
    for number in range(7):
        rows_here, cols_here = masters[number].shape
        scale = LEARN_RATE * 0.2 * math.sqrt(max(rows_here * devices_all, cols_here))
        turned = back[number, :rows_here, :cols_here].astype(jnp.float32)
        updated.append(masters[number] - scale * turned)
    tokens_all = tokens.shape[0] * devices_all
    gains_new = norm_gains - 0.1 / math.sqrt(tokens_all) * gains_moment
    return (
        block_out,
        tokens_grad,
        *grad_list,
        gains_grad,
        *updated,
        gains_new,
        *moments,
        gains_moment,
    )


def solution(mesh):
    return jax.shard_map(
        shards,
        mesh=mesh,
        in_specs=(
            P(("dp", "fsdp"), None),
            P(("dp", "fsdp"), None),
            P(("dp", "fsdp"), None),
            P(("dp", "fsdp"), None),
            P(("dp", "fsdp"), None),
            P(("dp", "fsdp"), None),
            P(("dp", "fsdp"), None),
            P(("dp", "fsdp"), None),
            P(("dp", "fsdp"), None),
            P(("dp", "fsdp"), None),
            P(("dp", "fsdp")),
            P(("dp", "fsdp"), None),
            P(("dp", "fsdp"), None),
            P(("dp", "fsdp"), None),
            P(("dp", "fsdp"), None),
            P(("dp", "fsdp"), None),
            P(("dp", "fsdp"), None),
            P(("dp", "fsdp"), None),
            P(("dp", "fsdp")),
        ),
        out_specs=(
            P(("dp", "fsdp"), None),
            P(("dp", "fsdp"), None),
            P(("dp", "fsdp"), None),
            P(("dp", "fsdp"), None),
            P(("dp", "fsdp"), None),
            P(("dp", "fsdp"), None),
            P(("dp", "fsdp"), None),
            P(("dp", "fsdp"), None),
            P(("dp", "fsdp"), None),
            P(("dp", "fsdp")),
            P(("dp", "fsdp"), None),
            P(("dp", "fsdp"), None),
            P(("dp", "fsdp"), None),
            P(("dp", "fsdp"), None),
            P(("dp", "fsdp"), None),
            P(("dp", "fsdp"), None),
            P(("dp", "fsdp"), None),
            P(("dp", "fsdp")),
            P(("dp", "fsdp"), None),
            P(("dp", "fsdp"), None),
            P(("dp", "fsdp"), None),
            P(("dp", "fsdp"), None),
            P(("dp", "fsdp"), None),
            P(("dp", "fsdp"), None),
            P(("dp", "fsdp"), None),
            P(("dp", "fsdp")),
        ),
        check_vma=False,
    )
```
